8 devices in a mesh: rep: 1 (over z), dp: 8 (over x, y, core).
Axes of the slice: x: 2, y: 2, z: 1, core: 2. Of those that a mesh axis runs over, the one named last changes fastest.
Arguments:
- x: bfloat16 [8, 2048, 1024], P(('rep', 'dp'))
- dy: bfloat16 [8, 2048, 1024], P(('rep', 'dp'))
- wq: bfloat16 [2, 1024, 1536], P(None, 'dp')
- wk: bfloat16 [2, 1024, 256], P(None, 'dp')
- wv: bfloat16 [2, 1024, 256], P(None, 'dp')
- wo: bfloat16 [2, 1536, 1024], P(None, 'dp')
- w_gate: bfloat16 [2, 1024, 4096], P(None, 'dp')
- w_up: bfloat16 [2, 1024, 4096], P(None, 'dp')
- w_down: bfloat16 [2, 4096, 1024], P(None, 'dp')
- m_wq: float32 [2, 1024, 1536], P(None, 'dp')
- m_wk: float32 [2, 1024, 256], P(None, 'dp')
- m_wv: float32 [2, 1024, 256], P(None, 'dp')
- m_wo: float32 [2, 1536, 1024], P(None, 'dp')
- m_w_gate: float32 [2, 1024, 4096], P(None, 'dp')
- m_w_up: float32 [2, 1024, 4096], P(None, 'dp')
- m_w_down: float32 [2, 4096, 1024], P(None, 'dp')
- v_wq: float32 [2, 1024, 1536], P(None, 'dp')
- v_wk: float32 [2, 1024, 256], P(None, 'dp')
- v_wv: float32 [2, 1024, 256], P(None, 'dp')
- v_wo: float32 [2, 1536, 1024], P(None, 'dp')
- v_w_gate: float32 [2, 1024, 4096], P(None, 'dp')
- v_w_up: float32 [2, 1024, 4096], P(None, 'dp')
- v_w_down: float32 [2, 4096, 1024], P(None, 'dp')
Outputs:
- output 1: bfloat16 [2, 1024, 1536], P('rep', 'dp')
- output 2: bfloat16 [2, 1024, 256], P('rep', 'dp')
- output 3: bfloat16 [2, 1024, 256], P('rep', 'dp')
- output 4: bfloat16 [2, 1536, 1024], P('rep', 'dp')
- output 5: bfloat16 [2, 1024, 4096], P('rep', 'dp')
- output 6: bfloat16 [2, 1024, 4096], P('rep', 'dp')
- output 7: bfloat16 [2, 4096, 1024], P('rep', 'dp')
- output 8: float32 [2, 1024, 1536], P('rep', 'dp')
- output 9: float32 [2, 1024, 256], P('rep', 'dp')
- output 10: float32 [2, 1024, 256], P('rep', 'dp')
- output 11: float32 [2, 1536, 1024], P('rep', 'dp')
- output 12: float32 [2, 1024, 4096], P('rep', 'dp')
- output 13: float32 [2, 1024, 4096], P('rep', 'dp')
- output 14: float32 [2, 4096, 1024], P('rep', 'dp')
- output 15: float32 [2, 1024, 1536], P('rep', 'dp')
- output 16: float32 [2, 1024, 256], P('rep', 'dp')
- output 17: float32 [2, 1024, 256], P('rep', 'dp')
- output 18: float32 [2, 1536, 1024], P('rep', 'dp')
- output 19: float32 [2, 1024, 4096], P('rep', 'dp')
- output 20: float32 [2, 1024, 4096], P('rep', 'dp')
- output 21: float32 [2, 4096, 1024], P('rep', 'dp')
All inputs are finite; a program needn't handle non-finite values.
Results may differ from the reference program's by a relative error of at most 0.024.
Values are sent between devices in bfloat16 or wider.
A program may use at most 2 GiB of HBM per device.

```python
import jax
import jax.numpy as jnp
from jax import lax

SEQUENCES = 8
TOKENS = 2048
D = 1024
HEADS = 12
KV_HEADS = 2
HEAD = 128
FF = 4096
LAYERS = 2
THETA = 10000
NAMES = ("wq", "wk", "wv", "wo", "w_gate", "w_up", "w_down")
SHAPES = {
    "wq": (LAYERS, D, HEADS * HEAD),
    "wk": (LAYERS, D, KV_HEADS * HEAD),
    "wv": (LAYERS, D, KV_HEADS * HEAD),
    "wo": (LAYERS, HEADS * HEAD, D),
    "w_gate": (LAYERS, D, FF),
    "w_up": (LAYERS, D, FF),
    "w_down": (LAYERS, FF, D),
}


def bump(key, n, height):
    away = (jnp.arange(n, dtype=jnp.int32) - jax.random.randint(key, (), 0, n, jnp.int32)) % n
    return jnp.where(away < n // 8, height, 1.0)


def together(key, own, strength):
    shared = jax.random.normal(key, own.shape[1:], jnp.float32)
    return (own + strength * shared) * lax.rsqrt(1 + strength * strength)


def setup_inputs(seed: int = 0, part: int = 0) -> dict:
    kx, kdy, ka, kb, kz, kf, kh, kl, *keys = jax.random.split(jax.random.key(seed), 8 + 3 * len(NAMES))
    kx, kdy, ka, kb = (jax.random.fold_in(k, part) for k in (kx, kdy, ka, kb))
    kw, km, kv = (keys[i::3] for i in range(3))
    shape = (SEQUENCES, TOKENS, D)
    much_x, much_dy = jax.random.uniform(kz, (2,), jnp.float32, 0.0, 1.0)
    loud = 2.0 ** jax.random.uniform(jax.random.fold_in(kz, 1), (), jnp.float32, -1.0, 2.0)
    layers = 2.0 ** jax.random.uniform(kl, (LAYERS, 1, 1), jnp.float32, -1.0, 1.0)
    times = {"wq": 1.0, "wk": 1.0, "wv": 2.0, "wo": layers, "w_gate": 1.0, "w_up": bump(kh, FF, 4.0), "w_down": layers}
    x = together(ka, jax.random.normal(kx, shape, jnp.float32), much_x) * bump(kf, D, 4.0)
    dy = together(kb, jax.random.normal(kdy, shape, jnp.float32), much_dy)
    drawn = {"x": x.astype(jnp.bfloat16), "dy": (loud * dy * (SEQUENCES * TOKENS) ** -0.5).astype(jnp.bfloat16)}
    for key, name in zip(kw, NAMES, strict=True):
        drawn[name] = (jax.random.normal(key, SHAPES[name], jnp.float32) * SHAPES[name][1] ** -0.5 * times[name]).astype(jnp.bfloat16)
    for key, name in zip(km, NAMES, strict=True):
        drawn[f"m_{name}"] = 0.1 * jax.random.normal(key, SHAPES[name], jnp.float32)
    for key, name in zip(kv, NAMES, strict=True):
        drawn[f"v_{name}"] = jax.random.uniform(key, SHAPES[name], jnp.float32, 0.02, 0.06)
    return drawn


def matmul(a, w):
    return jnp.dot(a, w, preferred_element_type=jnp.float32).astype(jnp.bfloat16)


def normed(h):
    wide = h.astype(jnp.float32)
    scale = lax.rsqrt(jnp.mean(wide**2, -1, keepdims=True) + 1e-6)
    return (wide * scale).astype(jnp.bfloat16)


def turned(t, theta):
    half = t.shape[-1] // 2
    angle = jnp.arange(t.shape[0], dtype=jnp.float32)[:, None] * theta ** (-jnp.arange(half, dtype=jnp.float32) / half)
    cos, sin = jnp.cos(angle)[:, None], jnp.sin(angle)[:, None]
    a, b = t[..., :half].astype(jnp.float32), t[..., half:].astype(jnp.float32)
    return jnp.concatenate([a * cos - b * sin, b * cos + a * sin], -1).astype(jnp.bfloat16)


def seen_by(q, k, v):
    tokens, kv = q.shape[0], k.shape[1]
    q = q.reshape(tokens, kv, -1, q.shape[-1])
    scores = jnp.einsum("tgsd,ugd->gstu", q.astype(jnp.float32), k.astype(jnp.float32)) * q.shape[-1] ** -0.5
    place = jnp.arange(tokens)
    weights = jax.nn.softmax(jnp.where(place[:, None] >= place, scores, -jnp.inf), -1).astype(jnp.bfloat16)
    return jnp.einsum("gstu,ugd->tgsd", weights.astype(jnp.float32), v.astype(jnp.float32)).astype(jnp.bfloat16).reshape(tokens, -1)


def layer(h, w):
    a = normed(h)
    q, k = (turned(matmul(a, w[name]).reshape(h.shape[0], -1, HEAD), THETA) for name in ("wq", "wk"))
    h = h + matmul(seen_by(q, k, matmul(a, w["wv"]).reshape(h.shape[0], -1, HEAD)), w["wo"])
    b = normed(h)
    gate = jnp.dot(b, w["w_gate"], preferred_element_type=jnp.float32)
    up = jnp.dot(b, w["w_up"], preferred_element_type=jnp.float32)
    return h + matmul((jax.nn.silu(gate) * up).astype(jnp.bfloat16), w["w_down"])


def adamw(w, m, v, g):
    m = 0.9 * m + 0.1 * g
    v = 0.95 * v + 0.05 * g * g
    step = m * lax.rsqrt(v + 1e-8) + 0.1 * w
    return (w - 0.02 * step).astype(jnp.bfloat16), m, v


def clipped(gradients, sum_of_squares, count):
    factor = jnp.minimum(1.0, 0.5 * lax.rsqrt(sum_of_squares / count + 1e-30))
    return [g * factor for g in gradients]


def stack(weights, h):
    return lax.scan(lambda h, w: (layer(h, w), None), h, weights)[0]


def reference(x, dy, wq, wk, wv, wo, w_gate, w_up, w_down, m_wq, m_wk, m_wv, m_wo, m_w_gate, m_w_up, m_w_down, v_wq, v_wk, v_wv, v_wo, v_w_gate, v_w_up, v_w_down):
    weights = dict(zip(NAMES, (wq, wk, wv, wo, w_gate, w_up, w_down), strict=True))

    def take(so_far, sequence):
        h, by_y = sequence
        _, back = jax.vjp(stack, weights, h)
        by_weights, by_h = back(by_y)
        return jax.tree.map(lambda total, term: total + term.astype(jnp.float32), so_far, by_weights), by_h

    none_yet = {name: jnp.zeros(w.shape, jnp.float32) for name, w in weights.items()}
    by_weights, by_x = lax.scan(take, none_yet, (x, dy))
    gradients = [by_weights[name].astype(jnp.bfloat16).astype(jnp.float32) for name in NAMES]
    gradients = clipped(gradients, sum(jnp.sum(g * g) for g in gradients), sum(g.size for g in gradients))
    first = (m_wq, m_wk, m_wv, m_wo, m_w_gate, m_w_up, m_w_down)
    second = (v_wq, v_wk, v_wv, v_wo, v_w_gate, v_w_up, v_w_down)
    new = [adamw(weights[name].astype(jnp.float32), m, v, g) for name, m, v, g in zip(NAMES, first, second, gradients, strict=True)]
    return tuple(one[which] for which in range(3) for one in new)
```

```python
import functools

import jax
import jax.numpy as jnp
from jax import lax
from jax.experimental import pallas as pl
from jax.experimental.pallas import tpu as pltpu
from jax.sharding import PartitionSpec as P

HEAD = 128
THETA = 10000
EPS = 1e-6
NEG = -1e30
HIDDEN = 2 * NEG
LOG2E = 1.4426950408889634
VMEM = 60 * 2**20
STRIP = 512


def dot(a, b, ca=1, cb=0):
    return lax.dot_general(a, b, (((ca,), (cb,)), ((), ())), preferred_element_type=jnp.float32)


def low(t):
    return t.astype(jnp.bfloat16)


def wide(t):
    return t.astype(jnp.float32)


def params(*semantics):
    return pltpu.CompilerParams(dimension_semantics=semantics, vmem_limit_bytes=VMEM)


def turn(x, cos, sin):
    return x * cos + pltpu.roll(x, HEAD // 2, 1) * sin


def gap_of(bk, cols, bq):
    return lax.rem(lax.broadcasted_iota(jnp.int32, (bk, cols), 1), bq) - lax.broadcasted_iota(jnp.int32, (bk, cols), 0)


def load_queries(q_ref, q_s, cos, sin, kv, g, bq):
    for i in range(kv):
        for n in range(g):
            at = (i * g + n) * HEAD
            x = wide(q_ref[:, at : at + HEAD])
            q_s[i, n * bq : (n + 1) * bq, :] = low(x if cos is None else turn(x, cos, sin))


def load_keys(k_ref, k_s, cos_ref, sin_ref, kv):
    for i in range(kv):
        k_s[i] = low(turn(wide(k_ref[:, i * HEAD : (i + 1) * HEAD]), cos_ref[...], sin_ref[...]))


def attend_kernel(q_ref, k_ref, v_ref, cos_ref, sin_ref, o_ref, lse_ref, q_s, k_s, v_s, top_s, mix_s, gap_s, *, kv, g, bq, bk, scale):
    iq = pl.program_id(0)
    cols, e = g * bq, scale * LOG2E
    strip = min(STRIP, cols)
    pieces = [(i, at) for i in range(kv) for at in range(0, cols, strip)]

    @pl.when(iq == 0)
    def _():
        gap_s[...] = gap_of(bk, cols, bq)
        load_keys(k_ref, k_s, cos_ref, sin_ref, kv)
        for i in range(kv):
            v_s[i, :HEAD, :] = v_ref[:, i * HEAD : (i + 1) * HEAD].T
            v_s[i, HEAD:, :] = jnp.ones((8, v_s.shape[2]), v_s.dtype)

    here = pl.ds(iq * bq, bq)
    load_queries(q_ref, q_s, cos_ref[here, :], sin_ref[here, :], kv, g, bq)
    top_s[...] = jnp.full(top_s.shape, NEG, jnp.float32)
    mix_s[...] = jnp.zeros(mix_s.shape, jnp.float32)

    def block(j, masked):
        keys = pl.ds(pl.multiple_of(j * bk, bk), bk)
        scores = [dot(k_s[i, keys, :], q_s[i, at : at + strip, :], 1, 1) for i, at in pieces]
        weights, keeps = [], []
        for (i, at), s in zip(pieces, scores):
            if masked:
                s = jnp.where(gap_s[:, at : at + strip] >= j * bk - iq * bq, s, HIDDEN)
            old = top_s[i : i + 1, at : at + strip]
            top = jnp.maximum(old, s.max(axis=0, keepdims=True))
            top_s[i : i + 1, at : at + strip] = top
            weights.append(low(jnp.exp2((s - top) * e)))
            keeps.append(jnp.exp2((old - top) * e))
        for (i, at), p, keep in zip(pieces, weights, keeps):
            mix_s[i, :, at : at + strip] = mix_s[i, :, at : at + strip] * keep + dot(v_s[i, :, keys], p, 1, 0)

    whole = lax.div(iq * bq + 1, bk)
    last = lax.div(iq * bq + bq - 1 + bk, bk)
    lax.fori_loop(0, whole, lambda j, _: block(j, False), None)
    lax.fori_loop(whole, last, lambda j, _: block(j, True), None)
    for i in range(kv):
        total = mix_s[i, HEAD : HEAD + 1, :]
        out = mix_s[i, :HEAD, :] * (1 / total)
        lse = top_s[i : i + 1, :] * scale + jnp.log(total)
        for n in range(g):
            at = (i * g + n) * HEAD
            o_ref[:, at : at + HEAD] = low(out[:, n * bq : (n + 1) * bq].T)
            lse_ref[i, n : n + 1, :] = lse[:, n * bq : (n + 1) * bq]


def attend(qkv, cos, sin, kv, g, bq=512, bk=512):
    tokens = qkv.shape[0]
    nq, nk = kv * g * HEAD, kv * HEAD
    flops = 2 * tokens * tokens * nq
    return pl.pallas_call(
        functools.partial(attend_kernel, kv=kv, g=g, bq=bq, bk=bk, scale=HEAD**-0.5),
        grid=(tokens // bq,),
        in_specs=[
            pl.BlockSpec((bq, nq), lambda i: (i, 0)),
            pl.BlockSpec((tokens, nk), lambda i: (0, nq // nk)),
            pl.BlockSpec((tokens, nk), lambda i: (0, nq // nk + 1)),
            pl.BlockSpec((tokens, HEAD), lambda i: (0, 0)),
            pl.BlockSpec((tokens, HEAD), lambda i: (0, 0)),
        ],
        out_specs=[pl.BlockSpec((bq, nq), lambda i: (i, 0)), pl.BlockSpec((kv, g, bq), lambda i: (0, 0, i))],
        out_shape=[jax.ShapeDtypeStruct((tokens, nq), jnp.bfloat16), jax.ShapeDtypeStruct((kv, g, tokens), jnp.float32)],
        scratch_shapes=[
            pltpu.VMEM((kv, g * bq, HEAD), jnp.bfloat16),
            pltpu.VMEM((kv, tokens, HEAD), jnp.bfloat16),
            pltpu.VMEM((kv, HEAD + 8, tokens), jnp.bfloat16),
            pltpu.VMEM((kv, g * bq), jnp.float32),
            pltpu.VMEM((kv, HEAD + 8, g * bq), jnp.float32),
            pltpu.VMEM((bk, g * bq), jnp.int32),
        ],
        compiler_params=params("arbitrary"),
        cost_estimate=pl.CostEstimate(flops=4 * flops, bytes_accessed=20 * 2**20, transcendentals=tokens * tokens * kv * g),
        name="attend",
    )(qkv, qkv, qkv, cos, sin)


def attend_back_kernel(q_ref, k_ref, v_ref, cos_ref, sin_ref, do_ref, o_ref, lse_ref, out_ref, q_s, do_s, k_s, dq_s, dk_s, dv_s, gap_s, *, kv, g, bq, bk, scale):
    iq = pl.program_id(0)
    cols, e = g * bq, scale * LOG2E
    strip = min(STRIP, cols)
    pieces = [(i, at) for i in range(kv) for at in range(0, cols, strip)]
    nq, nk = kv * g * HEAD, kv * HEAD

    @pl.when(iq == 0)
    def _():
        gap_s[...] = gap_of(bk, cols, bq)
        load_keys(k_ref, k_s, cos_ref, sin_ref, kv)
        dk_s[...] = jnp.zeros_like(dk_s)
        dv_s[...] = jnp.zeros_like(dv_s)

    here = pl.ds(iq * bq, bq)
    cos, sin = cos_ref[here, :], sin_ref[here, :]
    load_queries(q_ref, q_s, cos, sin, kv, g, bq)
    load_queries(do_ref, do_s, None, None, kv, g, bq)
    dq_s[...] = jnp.zeros_like(dq_s)
    lses, deltas = [], []
    for i in range(kv):
        one, two = [], []
        for n in range(g):
            at = (i * g + n) * HEAD
            one.append(lse_ref[i, n : n + 1, :])
            both = wide(do_ref[:, at : at + HEAD]) * wide(o_ref[:, at : at + HEAD])
            two.append(both.T.sum(axis=0, keepdims=True))
        lses.append(jnp.concatenate(one, axis=1) * LOG2E)
        deltas.append(jnp.concatenate(two, axis=1))

    def block(j, masked):
        keys = pl.ds(pl.multiple_of(j * bk, bk), bk)
        qs = [q_s[i, at : at + strip, :] for i, at in pieces]
        dos = [do_s[i, at : at + strip, :] for i, at in pieces]
        scores = [dot(k_s[i, keys, :], x, 1, 1) for (i, _), x in zip(pieces, qs)]
        dps = [dot(v_ref[keys, i * HEAD : (i + 1) * HEAD], x, 1, 1) for (i, _), x in zip(pieces, dos)]
        for n, (i, at) in enumerate(pieces):
            p = jnp.exp2(scores[n] * e - lses[i][:, at : at + strip])
            if masked:
                p = jnp.where(gap_s[:, at : at + strip] >= j * bk - iq * bq, p, 0.0)
            ds = low(p * (dps[n] - deltas[i][:, at : at + strip]))
            dv_s[i, keys, :] += dot(low(p), dos[n], 1, 0)
            dk_s[i, keys, :] += dot(ds, qs[n], 1, 0)
            dq_s[i, :, at : at + strip] += dot(k_s[i, keys, :].T, ds, 1, 0)

    whole = lax.div(iq * bq + 1, bk)
    last = lax.div(iq * bq + bq - 1 + bk, bk)
    lax.fori_loop(0, whole, lambda j, _: block(j, False), None)
    lax.fori_loop(whole, last, lambda j, _: block(j, True), None)
    for i in range(kv):
        for n in range(g):
            at = (i * g + n) * HEAD
            x = wide(low((dq_s[i, :, n * bq : (n + 1) * bq] * scale).T))
            out_ref[here, at : at + HEAD] = low(turn(x, cos, -sin))

    @pl.when(iq == pl.num_programs(0) - 1)
    def _():
        for i in range(kv):
            at = nq + i * HEAD
            out_ref[:, at : at + HEAD] = low(turn(wide(low(dk_s[i] * scale)), cos_ref[...], -sin_ref[...]))
            out_ref[:, at + nk : at + nk + HEAD] = low(dv_s[i])


def attend_back(qkv, cos, sin, d_out, out, lse, kv, g, bq=256, bk=256):
    tokens = qkv.shape[0]
    nq, nk = kv * g * HEAD, kv * HEAD
    rows = pl.BlockSpec((bq, nq), lambda i: (i, 0))
    table = pl.BlockSpec((tokens, HEAD), lambda i: (0, 0))
    return pl.pallas_call(
        functools.partial(attend_back_kernel, kv=kv, g=g, bq=bq, bk=bk, scale=HEAD**-0.5),
        grid=(tokens // bq,),
        in_specs=[
            rows,
            pl.BlockSpec((tokens, nk), lambda i: (0, nq // nk)),
            pl.BlockSpec((tokens, nk), lambda i: (0, nq // nk + 1)),
            table,
            table,
            rows,
            rows,
            pl.BlockSpec((kv, g, bq), lambda i: (0, 0, i)),
        ],
        out_specs=pl.BlockSpec(qkv.shape, lambda i: (0, 0)),
        out_shape=jax.ShapeDtypeStruct(qkv.shape, jnp.bfloat16),
        scratch_shapes=[
            pltpu.VMEM((kv, g * bq, HEAD), jnp.bfloat16),
            pltpu.VMEM((kv, g * bq, HEAD), jnp.bfloat16),
            pltpu.VMEM((kv, tokens, HEAD), jnp.bfloat16),
            pltpu.VMEM((kv, HEAD, g * bq), jnp.float32),
            pltpu.VMEM((kv, tokens, HEAD), jnp.float32),
            pltpu.VMEM((kv, tokens, HEAD), jnp.float32),
            pltpu.VMEM((bk, g * bq), jnp.int32),
        ],
        compiler_params=params("arbitrary"),
        cost_estimate=pl.CostEstimate(flops=10 * tokens * tokens * nq, bytes_accessed=40 * 2**20, transcendentals=tokens * tokens * kv * g),
        name="attend_back",
    )(qkv, qkv, qkv, cos, sin, d_out, out, lse)


TURN = 512


def unit_kernel(b_ref, w_ref, act_ref, slope_ref, *, rows):
    for at in range(0, b_ref.shape[0], rows):
        both = dot(b_ref[at : at + rows, :], w_ref[...])
        gate, up = both[:, :TURN], both[:, TURN:]
        sig = jax.nn.sigmoid(gate)
        silu = gate * sig
        act_ref[at : at + rows, :] = low(silu * up)
        slope_ref[at : at + rows, :TURN] = up * (sig + silu * (1 - sig))
        slope_ref[at : at + rows, TURN:] = silu


def unit(b, w, bm=2048, rows=256):
    tokens, d = b.shape
    n = w.shape[1] // (2 * TURN)
    return pl.pallas_call(
        functools.partial(unit_kernel, rows=rows),
        grid=(n, tokens // bm),
        in_specs=[pl.BlockSpec((bm, d), lambda j, i: (i, 0)), pl.BlockSpec((d, 2 * TURN), lambda j, i: (0, j))],
        out_specs=[pl.BlockSpec((bm, TURN), lambda j, i: (i, j)), pl.BlockSpec((bm, 2 * TURN), lambda j, i: (i, j))],
        out_shape=[jax.ShapeDtypeStruct((tokens, n * TURN), jnp.bfloat16), jax.ShapeDtypeStruct((tokens, 2 * n * TURN), jnp.float32)],
        compiler_params=params("arbitrary", "arbitrary"),
        cost_estimate=pl.CostEstimate(flops=2 * tokens * d * w.shape[1], bytes_accessed=tokens * n * TURN * 12, transcendentals=tokens * n * TURN),
        name="unit",
    )(b, w)


def unit_back_kernel(dy_ref, wd_ref, slope_ref, out_ref, *, rows):
    for at in range(0, dy_ref.shape[0], rows):
        by_act = wide(low(dot(dy_ref[at : at + rows, :], wd_ref[...], 1, 1)))
        out_ref[at : at + rows, :TURN] = low(by_act * slope_ref[at : at + rows, :TURN])
        out_ref[at : at + rows, TURN:] = low(by_act * slope_ref[at : at + rows, TURN:])


def unit_back(dy, wd, both, bm=2048, rows=256):
    tokens, d = dy.shape
    n = wd.shape[0] // TURN
    pair = pl.BlockSpec((bm, 2 * TURN), lambda j, i: (i, j))
    return pl.pallas_call(
        functools.partial(unit_back_kernel, rows=rows),
        grid=(n, tokens // bm),
        in_specs=[pl.BlockSpec((bm, d), lambda j, i: (i, 0)), pl.BlockSpec((TURN, d), lambda j, i: (j, 0)), pair],
        out_specs=pair,
        out_shape=jax.ShapeDtypeStruct(both.shape, jnp.bfloat16),
        compiler_params=params("arbitrary", "arbitrary"),
        cost_estimate=pl.CostEstimate(flops=2 * tokens * d * wd.shape[0], bytes_accessed=tokens * wd.shape[0] * 12, transcendentals=tokens * wd.shape[0]),
        name="unit_back",
    )(dy, wd, both)


def barrier(*values):
    return lax.optimization_barrier(values)


def scale_of(h):
    return lax.rsqrt(jnp.mean(wide(h) ** 2, -1, keepdims=True) + EPS)


def normed(h):
    return low(wide(h) * scale_of(h))


def normed_back(h, by_out, by_h):
    x, g, scale = wide(h), wide(by_out), scale_of(h)
    through = g * scale - x * (scale**3 * jnp.mean(g * x, -1, keepdims=True))
    return low(wide(by_h) + through)


def tables(tokens):
    half = HEAD // 2
    angle = jnp.arange(tokens, dtype=jnp.float32)[:, None] * THETA ** (-jnp.arange(half, dtype=jnp.float32) / half)
    cos, sin = jnp.cos(angle), jnp.sin(angle)
    return jnp.concatenate([cos, cos], 1), jnp.concatenate([-sin, sin], 1)


def side_by_side_kernel(*refs, size):
    *parts, out_ref = refs
    to = 0
    for at in range(0, parts[0].shape[2], size or parts[0].shape[2]):
        for part in parts:
            n = size or part.shape[2]
            out_ref[:, to : to + n] = part[0, :, at : at + n]
            to += n


def side_by_side(parts, number, size=None):
    rows = parts[0].shape[1]
    columns = sum(t.shape[2] for t in parts)
    return pl.pallas_call(
        functools.partial(side_by_side_kernel, size=size),
        grid=(2,),
        in_specs=[pl.BlockSpec((1, rows // 2, t.shape[2]), lambda i: (number, i, 0)) for t in parts],
        out_specs=pl.BlockSpec((rows // 2, columns), lambda i: (i, 0)),
        out_shape=jax.ShapeDtypeStruct((rows, columns), parts[0].dtype),
        compiler_params=params("arbitrary"),
        name="side_by_side",
    )(*parts)


def total_kernel(mine_ref, out_ref, all_s, send_sem, recv_sem, *, n):
    me = lax.axis_index("dp")
    entry = pltpu.get_barrier_semaphore()
    for k in range(1, n):
        pl.semaphore_signal(entry, inc=1, device_id={"dp": lax.rem(me + k, n)}, device_id_type=pl.DeviceIdType.MESH)
    pl.semaphore_wait(entry, n - 1)
    copies = []
    for k in range(1, n):
        copies.append(
            pltpu.make_async_remote_copy(
                src_ref=mine_ref,
                dst_ref=all_s.at[k],
                send_sem=send_sem.at[k],
                recv_sem=recv_sem.at[k],
                device_id={"dp": lax.rem(me + k, n)},
                device_id_type=pl.DeviceIdType.MESH,
            )
        )
    for copy in copies:
        copy.start()
    for copy in copies:
        copy.wait()
    total = mine_ref[...]
    for k in range(1, n):
        total = total + all_s[k]
    out_ref[...] = total


def total_of(mine, n):
    return pl.pallas_call(
        functools.partial(total_kernel, n=n),
        in_specs=[pl.BlockSpec(memory_space=pltpu.VMEM)],
        out_specs=pl.BlockSpec(memory_space=pltpu.VMEM),
        out_shape=jax.ShapeDtypeStruct((8, 128), jnp.float32),
        scratch_shapes=[pltpu.VMEM((n, 8, 128), jnp.float32), pltpu.SemaphoreType.DMA((n,)), pltpu.SemaphoreType.DMA((n,))],
        compiler_params=pltpu.CompilerParams(collective_id=0, has_side_effects=True),
        name="total",
    )(jnp.broadcast_to(mine, (8, 128)))


def update_kernel(squares_ref, *refs, layers, count, places):
    grads, refs = [refs[4 * n : 4 * n + 4] for n in range(layers)], refs[4 * layers :]
    weights, ms, vs, new_weights, new_ms, new_vs = (refs[i : i + 7] for i in range(0, 42, 7))
    factor = jnp.minimum(1.0, 0.5 * lax.rsqrt(squares_ref[:1, :1] / count + 1e-30))
    for n in range(layers):

        @pl.when(pl.program_id(0) == n)
        def _(n=n):
            for i, (which, runs) in enumerate(places):
                to = 0
                for at, size in runs:
                    here = pl.ds(to, size)
                    g = wide(grads[n][which][:, at : at + size]) * factor
                    m = 0.9 * ms[i][0, :, here] + 0.1 * g
                    v = 0.95 * vs[i][0, :, here] + 0.05 * g * g
                    w = wide(weights[i][0, :, here])
                    new_ms[i][0, :, here] = m
                    new_vs[i][0, :, here] = v
                    new_weights[i][0, :, here] = low(w - 0.02 * (m * lax.rsqrt(v + 1e-8) + 0.1 * w))
                    to += size


def update(squares, grads, weights, m, v, count, places, steps=8):
    layers = len(grads)

    def block(t):
        return pl.BlockSpec((1, t.shape[1] // steps, t.shape[2]), lambda n, i: (n, i, 0))

    def summed(t, n):
        return pl.BlockSpec((t.shape[0] // steps, t.shape[1]), lambda l, i: (jnp.where(l == n, i, jnp.where(l < n, 0, steps - 1)), 0))

    out = pl.pallas_call(
        functools.partial(update_kernel, layers=layers, count=count, places=places),
        grid=(layers, steps),
        in_specs=[pl.BlockSpec((8, 128), lambda n, i: (0, 0))]
        + [summed(t, n) for n, four in enumerate(grads) for t in four]
        + [block(t) for t in (*weights, *m, *v)],
        out_specs=[block(t) for t in (*weights, *m, *v)],
        out_shape=[jax.ShapeDtypeStruct(t.shape, t.dtype) for t in (*weights, *m, *v)],
        compiler_params=params("arbitrary", "arbitrary"),
        name="update",
    )(squares, *(t for four in grads for t in four), *weights, *m, *v)
    return tuple(out)


def solution(mesh):
    group = mesh.shape["dp"]

    def gather(w):
        return lax.all_gather(w, "dp", axis=0, tiled=True)

    def scatter(g):
        return lax.psum_scatter(g, "dp", scatter_dimension=0, tiled=True)

    def step(x, dy, *arrays):
        weights, m, v = (arrays[i : i + 7] for i in (0, 7, 14))
        wq, wk, wv, wo, wg, wu, wd = weights
        layers = wq.shape[0]
        nq, nk = wq.shape[2], wk.shape[2]
        kv, g = nk // HEAD, nq // nk
        full = []
        for n in range(layers):
            full.append((gather(side_by_side((wq, wk, wv), n)), gather(wo[n]), gather(side_by_side((wg, wu), n, TURN)), gather(wd[n])))
        h = x[0]
        cos, sin = tables(h.shape[0])
        kept = []
        for n in range(layers):
            wqkv, wo_, wgu, wd_ = full[n]
            a = normed(h)
            qkv = low(dot(a, wqkv))
            o, lse = attend(qkv, cos, sin, kv, g)
            mid = h + low(dot(o, wo_))
            b = normed(mid)
            act, slope = unit(b, wgu)
            kept.append((h, a, qkv, lse, o, mid, b, act, slope))
            if n < layers - 1:
                h = mid + low(dot(act, wd_))
        by_h = dy[0]
        mine = [None] * layers
        late = []
        for n in reversed(range(layers)):
            wqkv, wo_, wgu, wd_ = full[n]
            h, a, qkv, lse, o, mid, b, act, slope = kept[n]
            by_wd = low(dot(act, by_h, 0, 0))
            by_h, by_wd = barrier(by_h, by_wd)
            got_wd = scatter(by_wd)
            by_gu = unit_back(by_h, wd_, slope)
            if late:
                by_gu, late[1] = barrier(by_gu, late[1])
            by_wgu = low(dot(b, by_gu, 0, 0))
            if late:
                by_wgu, late[0] = barrier(by_wgu, late[0])
                mine[n + 1] = tuple(late)
            by_gu, by_wgu = barrier(by_gu, by_wgu)
            got_wgu = scatter(by_wgu)
            by_b = low(dot(by_gu, wgu, 1, 1))
            by_b, got_wd = barrier(by_b, got_wd)
            by_mid = normed_back(mid, by_b, by_h)
            by_wo = low(dot(o, by_mid, 0, 0))
            by_mid, by_wo = barrier(by_mid, by_wo)
            got_wo = scatter(by_wo)
            by_o = low(dot(by_mid, wo_, 1, 1))
            by_qkv = attend_back(qkv, cos, sin, by_o, o, lse, kv, g)
            by_qkv, got_wgu = barrier(by_qkv, got_wgu)
            by_wqkv = low(dot(a, by_qkv, 0, 0))
            if n:
                by_qkv, by_wqkv = barrier(by_qkv, by_wqkv)
                late = [scatter(by_wqkv), got_wo, got_wgu, got_wd]
                by_a = low(dot(by_qkv, wqkv, 1, 1))
                by_h = normed_back(h, by_a, by_mid)
            else:
                by_wqkv, got_wo = barrier(by_wqkv, got_wo)
                mine[n] = (scatter(by_wqkv), got_wo, got_wgu, got_wd)
        squares = sum(jnp.sum(wide(t) ** 2) for four in mine for t in four)
        count = group * sum(w.size for w in weights)
        ff = wg.shape[2]
        places = ((0, ((0, nq),)), (0, ((nq, nk),)), (0, ((nq + nk, nk),)), (1, ((0, wo.shape[2]),)))
        places += tuple((2, tuple((at, TURN) for at in range(first, 2 * ff, 2 * TURN))) for first in (0, TURN))
        places += ((3, ((0, wd.shape[2]),)),)
        return update(total_of(squares, group), mine, weights, m, v, count, places)

    states, cut = P(("rep", "dp"), None, None), P(None, "dp", None)
    return jax.shard_map(
        step,
        mesh=mesh,
        in_specs=(states, states) + (cut,) * 21,
        out_specs=(P("rep", "dp", None),) * 21,
        check_vma=False,
    )
```

```python
import functools

import jax
import jax.numpy as jnp
from jax import lax
from jax.experimental import pallas as pl
from jax.experimental.pallas import tpu as pltpu
from jax.sharding import PartitionSpec as P

HEAD = 128
THETA = 10000
EPS = 1e-6
NEG = -1e30
HIDDEN = 2 * NEG
LOG2E = 1.4426950408889634
VMEM = 60 * 2**20


def dot(a, b, ca=1, cb=0):
    return lax.dot_general(a, b, (((ca,), (cb,)), ((), ())), preferred_element_type=jnp.float32)


def low(t):
    return t.astype(jnp.bfloat16)


def wide(t):
    return t.astype(jnp.float32)


def params(*semantics):
    return pltpu.CompilerParams(dimension_semantics=semantics, vmem_limit_bytes=VMEM)


def turn(x, cos, sin):
    return x * cos + pltpu.roll(x, HEAD // 2, 1) * sin


def gap_of(bk, cols, bq):
    return lax.rem(lax.broadcasted_iota(jnp.int32, (bk, cols), 1), bq) - lax.broadcasted_iota(jnp.int32, (bk, cols), 0)


def load_queries(q_ref, q_s, cos, sin, kv, g, part):
    for i in range(kv):
        for s in range(q_ref.shape[0] // part):
            for n in range(g):
                at, to, rows = (i * g + n) * HEAD, (s * g + n) * part, slice(s * part, (s + 1) * part)
                x = q_ref[rows, at : at + HEAD]
                q_s[i, to : to + part, :] = x if cos is None else low(turn(wide(x), cos[rows], sin[rows]))


def load_keys(k_ref, k_s, cos_ref, sin_ref, kv):
    for i in range(kv):
        k_s[i] = low(turn(wide(k_ref[:, i * HEAD : (i + 1) * HEAD]), cos_ref[...], sin_ref[...]))


def attend_kernel(q_ref, k_ref, v_ref, cos_ref, sin_ref, o_ref, lse_ref, q_s, k_s, v_s, top_s, mix_s, gap_s, *, kv, g, bq, part, strip, dstrip, scale):
    iq = pl.program_id(0)
    cols, e = g * bq, scale * LOG2E

    @pl.when(iq == 0)
    def _():
        gap_s[...] = gap_of(part, g * part, part)
        load_keys(k_ref, k_s, cos_ref, sin_ref, kv)
        for i in range(kv):
            v_s[i, :HEAD, :] = v_ref[:, i * HEAD : (i + 1) * HEAD].T
            v_s[i, HEAD:, :] = jnp.ones((8, v_s.shape[2]), v_s.dtype)

    here = pl.ds(iq * bq, bq)
    load_queries(q_ref, q_s, cos_ref[here, :], sin_ref[here, :], kv, g, part)
    top_s[...] = jnp.full(top_s.shape, NEG, jnp.float32)
    mix_s[...] = jnp.zeros(mix_s.shape, jnp.float32)

    def work(j, pieces):
        scores = []
        for i, at, size, keys, edge in pieces:
            scores.append(dot(k_s[i, pl.ds(pl.multiple_of(j * bq, bq), keys), :], q_s[i, at : at + size, :], 1, 1))
        weights, keeps = [], []
        for (i, at, size, keys, edge), s in zip(pieces, scores):
            if edge:
                col = at % (g * part)
                tail = jnp.where(gap_s[:, col : col + size] >= 0, s[keys - part :], HIDDEN)
                s = tail if keys == part else jnp.concatenate([s[: keys - part], tail], 0)
            old = top_s[i : i + 1, at : at + size]
            top = jnp.maximum(old, s.max(axis=0, keepdims=True))
            top_s[i : i + 1, at : at + size] = top
            weights.append(low(jnp.exp2((s - top) * e)))
            keeps.append(jnp.exp2((old - top) * e))
        for (i, at, size, keys, edge), p, keep in zip(pieces, weights, keeps):
            values = v_s[i, :, pl.ds(pl.multiple_of(j * bq, bq), keys)]
            mix_s[i, :, at : at + size] = mix_s[i, :, at : at + size] * keep + dot(values, p, 1, 0)

    plain = [(i, at, strip, bq, False) for i in range(kv) for at in range(0, cols, strip)]
    lax.fori_loop(0, iq, lambda j, _: work(j, plain), None)
    work(iq, [(i, at, dstrip, (at // (g * part) + 1) * part, True) for i in range(kv) for at in range(0, cols, dstrip)])
    for i in range(kv):
        total = mix_s[i, HEAD : HEAD + 1, :]
        out = mix_s[i, :HEAD, :] * (1 / total)
        lse = top_s[i : i + 1, :] * scale + jnp.log(total)
        for s in range(bq // part):
            for n in range(g):
                at, to, rows = (i * g + n) * HEAD, (s * g + n) * part, slice(s * part, (s + 1) * part)
                o_ref[rows, at : at + HEAD] = low(out[:, to : to + part].T)
                lse_ref[i, n : n + 1, rows] = lse[:, to : to + part]


def attend(qkv, cos, sin, kv, g, bq=512, part=128, strip=512, dstrip=768):
    tokens = qkv.shape[0]
    nq, nk = kv * g * HEAD, kv * HEAD
    flops = 2 * tokens * tokens * nq
    return pl.pallas_call(
        functools.partial(attend_kernel, kv=kv, g=g, bq=bq, part=part, strip=strip, dstrip=dstrip, scale=HEAD**-0.5),
        grid=(tokens // bq,),
        in_specs=[
            pl.BlockSpec((bq, nq), lambda i: (i, 0)),
            pl.BlockSpec((tokens, nk), lambda i: (0, nq // nk)),
            pl.BlockSpec((tokens, nk), lambda i: (0, nq // nk + 1)),
            pl.BlockSpec((tokens, HEAD), lambda i: (0, 0)),
            pl.BlockSpec((tokens, HEAD), lambda i: (0, 0)),
        ],
        out_specs=[pl.BlockSpec((bq, nq), lambda i: (i, 0)), pl.BlockSpec((kv, g, bq), lambda i: (0, 0, i))],
        out_shape=[jax.ShapeDtypeStruct((tokens, nq), jnp.bfloat16), jax.ShapeDtypeStruct((kv, g, tokens), jnp.float32)],
        scratch_shapes=[
            pltpu.VMEM((kv, g * bq, HEAD), jnp.bfloat16),
            pltpu.VMEM((kv, tokens, HEAD), jnp.bfloat16),
            pltpu.VMEM((kv, HEAD + 8, tokens), jnp.bfloat16),
            pltpu.VMEM((kv, g * bq), jnp.float32),
            pltpu.VMEM((kv, HEAD + 8, g * bq), jnp.float32),
            pltpu.VMEM((part, g * part), jnp.int32),
        ],
        compiler_params=params("arbitrary"),
        cost_estimate=pl.CostEstimate(flops=4 * flops, bytes_accessed=20 * 2**20, transcendentals=tokens * tokens * kv * g),
        name="attend",
    )(qkv, qkv, qkv, cos, sin)


def attend_back_kernel(q_ref, k_ref, v_ref, cos_ref, sin_ref, do_ref, o_ref, lse_ref, out_ref, q_s, do_s, k_s, kt_s, dq_s, dk_s, dv_s, gap_s, *, kv, g, bq, part, strip, dstrip, scale):
    iq = pl.program_id(0)
    cols, e = g * bq, scale * LOG2E
    nq, nk = kv * g * HEAD, kv * HEAD

    @pl.when(iq == 0)
    def _():
        gap_s[...] = gap_of(part, g * part, part)
        load_keys(k_ref, k_s, cos_ref, sin_ref, kv)
        for i in range(kv):
            kt_s[i] = k_s[i].T
        dk_s[...] = jnp.zeros_like(dk_s)
        dv_s[...] = jnp.zeros_like(dv_s)

    here = pl.ds(iq * bq, bq)
    cos, sin = cos_ref[here, :], sin_ref[here, :]
    load_queries(q_ref, q_s, cos, sin, kv, g, part)
    load_queries(do_ref, do_s, None, None, kv, g, part)
    dq_s[...] = jnp.zeros_like(dq_s)
    lses, deltas = [], []
    for i in range(kv):
        one, two = [], []
        for s in range(bq // part):
            for n in range(g):
                at, rows = (i * g + n) * HEAD, slice(s * part, (s + 1) * part)
                one.append(lse_ref[i, n : n + 1, rows])
                both = wide(do_ref[rows, at : at + HEAD]) * wide(o_ref[rows, at : at + HEAD])
                two.append(both.T.sum(axis=0, keepdims=True))
        lses.append(jnp.concatenate(one, axis=1) * LOG2E)
        deltas.append(jnp.concatenate(two, axis=1))

    def work(j, pieces):
        base = pl.multiple_of(j * bq, bq)
        qs = [q_s[i, at : at + size, :] for i, at, size, _, _ in pieces]
        dos = [do_s[i, at : at + size, :] for i, at, size, _, _ in pieces]
        scores = [dot(k_s[i, pl.ds(base, keys), :], x, 1, 1) for (i, _, _, keys, _), x in zip(pieces, qs)]
        dps = [dot(v_ref[pl.ds(base, keys), i * HEAD : (i + 1) * HEAD], x, 1, 1) for (i, _, _, keys, _), x in zip(pieces, dos)]
        for n, (i, at, size, keys, edge) in enumerate(pieces):
            here_ = pl.ds(base, keys)
            p = jnp.exp2(scores[n] * e - lses[i][:, at : at + size])
            if edge:
                col = at % (g * part)
                tail = jnp.where(gap_s[:, col : col + size] >= 0, p[keys - part :], 0.0)
                p = tail if keys == part else jnp.concatenate([p[: keys - part], tail], 0)
            ds = low(p * (dps[n] - deltas[i][:, at : at + size]))
            dv_s[i, here_, :] += dot(low(p), dos[n], 1, 0)
            dk_s[i, here_, :] += dot(ds, qs[n], 1, 0)
            dq_s[i, :, at : at + size] += dot(kt_s[i, :, here_], ds, 1, 0)

    plain = [(i, at, strip, bq, False) for i in range(kv) for at in range(0, cols, strip)]
    lax.fori_loop(0, iq, lambda j, _: work(j, plain), None)
    work(iq, [(i, at, dstrip, (at // (g * part) + 1) * part, True) for i in range(kv) for at in range(0, cols, dstrip)])
    for i in range(kv):
        for s in range(bq // part):
            for n in range(g):
                at, to = (i * g + n) * HEAD, (s * g + n) * part
                x = wide(low((dq_s[i, :, to : to + part] * scale).T))
                rows = slice(s * part, (s + 1) * part)
                out_ref[pl.ds(iq * bq + s * part, part), at : at + HEAD] = low(turn(x, cos[rows], -sin[rows]))

    @pl.when(iq == pl.num_programs(0) - 1)
    def _():
        for i in range(kv):
            at = nq + i * HEAD
            out_ref[:, at : at + HEAD] = low(turn(wide(low(dk_s[i] * scale)), cos_ref[...], -sin_ref[...]))
            out_ref[:, at + nk : at + nk + HEAD] = low(dv_s[i])


def attend_back(qkv, cos, sin, d_out, out, lse, kv, g, bq=256, part=128, strip=256, dstrip=256):
    tokens = qkv.shape[0]
    nq, nk = kv * g * HEAD, kv * HEAD
    rows = pl.BlockSpec((bq, nq), lambda i: (i, 0))
    table = pl.BlockSpec((tokens, HEAD), lambda i: (0, 0))
    return pl.pallas_call(
        functools.partial(attend_back_kernel, kv=kv, g=g, bq=bq, part=part, strip=strip, dstrip=dstrip, scale=HEAD**-0.5),
        grid=(tokens // bq,),
        in_specs=[
            rows,
            pl.BlockSpec((tokens, nk), lambda i: (0, nq // nk)),
            pl.BlockSpec((tokens, nk), lambda i: (0, nq // nk + 1)),
            table,
            table,
            rows,
            rows,
            pl.BlockSpec((kv, g, bq), lambda i: (0, 0, i)),
        ],
        out_specs=pl.BlockSpec(qkv.shape, lambda i: (0, 0)),
        out_shape=jax.ShapeDtypeStruct(qkv.shape, jnp.bfloat16),
        scratch_shapes=[
            pltpu.VMEM((kv, g * bq, HEAD), jnp.bfloat16),
            pltpu.VMEM((kv, g * bq, HEAD), jnp.bfloat16),
            pltpu.VMEM((kv, tokens, HEAD), jnp.bfloat16),
            pltpu.VMEM((kv, HEAD, tokens), jnp.bfloat16),
            pltpu.VMEM((kv, HEAD, g * bq), jnp.float32),
            pltpu.VMEM((kv, tokens, HEAD), jnp.float32),
            pltpu.VMEM((kv, tokens, HEAD), jnp.float32),
            pltpu.VMEM((part, g * part), jnp.int32),
        ],
        compiler_params=params("arbitrary"),
        cost_estimate=pl.CostEstimate(flops=10 * tokens * tokens * nq, bytes_accessed=40 * 2**20, transcendentals=tokens * tokens * kv * g),
        name="attend_back",
    )(qkv, qkv, qkv, cos, sin, d_out, out, lse)


TURN = 512


def unit_kernel(b_ref, w_ref, act_ref, slope_ref, *, rows):
    for at in range(0, b_ref.shape[0], rows):
        both = dot(b_ref[at : at + rows, :], w_ref[...])
        gate, up = both[:, :TURN], both[:, TURN:]
        sig = jax.nn.sigmoid(gate)
        silu = gate * sig
        act_ref[at : at + rows, :] = low(silu * up)
        slope_ref[at : at + rows, :TURN] = up * (sig + silu * (1 - sig))
        slope_ref[at : at + rows, TURN:] = silu


def unit(b, w, bm=2048, rows=256):
    tokens, d = b.shape
    n = w.shape[1] // (2 * TURN)
    return pl.pallas_call(
        functools.partial(unit_kernel, rows=rows),
        grid=(n, tokens // bm),
        in_specs=[pl.BlockSpec((bm, d), lambda j, i: (i, 0)), pl.BlockSpec((d, 2 * TURN), lambda j, i: (0, j))],
        out_specs=[pl.BlockSpec((bm, TURN), lambda j, i: (i, j)), pl.BlockSpec((bm, 2 * TURN), lambda j, i: (i, j))],
        out_shape=[jax.ShapeDtypeStruct((tokens, n * TURN), jnp.bfloat16), jax.ShapeDtypeStruct((tokens, 2 * n * TURN), jnp.float32)],
        compiler_params=params("arbitrary", "arbitrary"),
        cost_estimate=pl.CostEstimate(flops=2 * tokens * d * w.shape[1], bytes_accessed=tokens * n * TURN * 12, transcendentals=tokens * n * TURN),
        name="unit",
    )(b, w)


def unit_back_kernel(dy_ref, wd_ref, slope_ref, b_ref, by_both_ref, by_w_ref, b_s, *, rows):
    @pl.when(pl.program_id(0) == 0)
    def _():
        b_s[...] = b_ref[...].T

    for at in range(0, dy_ref.shape[0], rows):
        by_act = wide(low(dot(dy_ref[at : at + rows, :], wd_ref[...], 1, 1)))
        by_both_ref[at : at + rows, :TURN] = low(by_act * slope_ref[at : at + rows, :TURN])
        by_both_ref[at : at + rows, TURN:] = low(by_act * slope_ref[at : at + rows, TURN:])
    for at in range(0, b_s.shape[0], rows):
        by_w_ref[at : at + rows, :] = low(dot(b_s[at : at + rows, :], by_both_ref[...]))


def unit_back(dy, wd, slope, b, rows=256):
    tokens, d = dy.shape
    n = wd.shape[0] // TURN
    whole = pl.BlockSpec((tokens, d), lambda j: (0, 0))
    pair = pl.BlockSpec((tokens, 2 * TURN), lambda j: (0, j))
    return pl.pallas_call(
        functools.partial(unit_back_kernel, rows=rows),
        grid=(n,),
        in_specs=[whole, pl.BlockSpec((TURN, d), lambda j: (j, 0)), pair, whole],
        out_specs=[pair, pl.BlockSpec((d, 2 * TURN), lambda j: (0, j))],
        out_shape=[jax.ShapeDtypeStruct(slope.shape, jnp.bfloat16), jax.ShapeDtypeStruct((d, slope.shape[1]), jnp.bfloat16)],
        scratch_shapes=[pltpu.VMEM((d, tokens), jnp.bfloat16)],
        compiler_params=params("arbitrary"),
        cost_estimate=pl.CostEstimate(flops=6 * tokens * d * wd.shape[0], bytes_accessed=tokens * wd.shape[0] * 14, transcendentals=0),
        name="unit_back",
    )(dy, wd, slope, b)


def barrier(*values):
    return lax.optimization_barrier(values)


def scale_of(h):
    return lax.rsqrt(jnp.mean(wide(h) ** 2, -1, keepdims=True) + EPS)


def normed(h):
    return low(wide(h) * scale_of(h))


def normed_back(h, by_out, by_h):
    x, g, scale = wide(h), wide(by_out), scale_of(h)
    through = g * scale - x * (scale**3 * jnp.mean(g * x, -1, keepdims=True))
    return low(wide(by_h) + through)


def tables(tokens):
    half = HEAD // 2
    angle = jnp.arange(tokens, dtype=jnp.float32)[:, None] * THETA ** (-jnp.arange(half, dtype=jnp.float32) / half)
    cos, sin = jnp.cos(angle), jnp.sin(angle)
    return jnp.concatenate([cos, cos], 1), jnp.concatenate([-sin, sin], 1)


def in_turns_kernel(a_ref, b_ref, out_ref):
    for at in range(0, a_ref.shape[2], TURN):
        out_ref[:, 2 * at : 2 * at + TURN] = a_ref[0, :, at : at + TURN]
        out_ref[:, 2 * at + TURN : 2 * at + 2 * TURN] = b_ref[0, :, at : at + TURN]


def in_turns(a, b, number):
    rows, columns = a.shape[1], a.shape[2]
    half = pl.BlockSpec((1, rows // 2, columns), lambda i: (number, i, 0))
    return pl.pallas_call(
        in_turns_kernel,
        grid=(2,),
        in_specs=[half, half],
        out_specs=pl.BlockSpec((rows // 2, 2 * columns), lambda i: (i, 0)),
        out_shape=jax.ShapeDtypeStruct((rows, 2 * columns), a.dtype),
        compiler_params=params("arbitrary"),
        name="in_turns",
    )(a, b)


def stack_kernel(*refs):
    *parts, below_ref, out_ref = refs
    rows, width = parts[0].shape[1], out_ref.shape[1]
    to = 0
    for part in parts:
        for at in range(0, part.shape[2], HEAD):
            piece, column = divmod(to, width)
            out_ref[piece * rows : (piece + 1) * rows, column : column + HEAD] = part[0, :, at : at + HEAD]
            to += HEAD
    out_ref[to // width * rows :, :] = below_ref[0]


def stack(parts, below, number):
    rows, width = parts[0].shape[1], below.shape[2]
    height = rows * sum(t.shape[2] for t in parts) // width + below.shape[1]
    return pl.pallas_call(
        stack_kernel,
        grid=(1,),
        in_specs=[pl.BlockSpec((1, *t.shape[1:]), lambda i: (number, 0, 0)) for t in (*parts, below)],
        out_specs=pl.BlockSpec((height, width), lambda i: (0, 0)),
        out_shape=jax.ShapeDtypeStruct((height, width), below.dtype),
        compiler_params=params("arbitrary"),
        name="stack",
    )(*parts, below)


def unstack(t, rows, columns):
    group, _, width = t.shape
    pieces = [t[:, at : at + rows].reshape(group * rows, width) for at in range(0, rows * columns // width, rows)]
    return jnp.concatenate(pieces, 1), t[:, rows * columns // width :].reshape(-1, width)


def total_kernel(last_ref, rest_ref, out_ref, mine_s, all_s, send_sem, recv_sem, *, n):
    me = lax.axis_index("dp")
    last = wide(last_ref[...])
    mine_s[...] = rest_ref[...] + jnp.sum(last * last, keepdims=True)
    entry = pltpu.get_barrier_semaphore()
    for k in range(1, n):
        pl.semaphore_signal(entry, inc=1, device_id={"dp": lax.rem(me + k, n)}, device_id_type=pl.DeviceIdType.MESH)
    pl.semaphore_wait(entry, n - 1)
    copies = []
    for k in range(1, n):
        copies.append(
            pltpu.make_async_remote_copy(
                src_ref=mine_s,
                dst_ref=all_s.at[k],
                send_sem=send_sem.at[k],
                recv_sem=recv_sem.at[k],
                device_id={"dp": lax.rem(me + k, n)},
                device_id_type=pl.DeviceIdType.MESH,
            )
        )
    for copy in copies:
        copy.start()
    for copy in copies:
        copy.wait()
    total = mine_s[...]
    for k in range(1, n):
        total = total + all_s[k]
    out_ref[...] = total


def total_of(last, rest, n):
    return pl.pallas_call(
        functools.partial(total_kernel, n=n),
        in_specs=[pl.BlockSpec(memory_space=pltpu.VMEM)] * 2,
        out_specs=pl.BlockSpec(memory_space=pltpu.VMEM),
        out_shape=jax.ShapeDtypeStruct((8, 128), jnp.float32),
        scratch_shapes=[
            pltpu.VMEM((8, 128), jnp.float32),
            pltpu.VMEM((n, 8, 128), jnp.float32),
            pltpu.SemaphoreType.DMA((n,)),
            pltpu.SemaphoreType.DMA((n,)),
        ],
        compiler_params=pltpu.CompilerParams(collective_id=0, has_side_effects=True),
        name="total",
    )(last, jnp.broadcast_to(rest, (8, 128)))


def update_kernel(squares_ref, *refs, layers, count, places):
    grads, refs = [refs[4 * n : 4 * n + 4] for n in range(layers)], refs[4 * layers :]
    weights, ms, vs, new_weights, new_ms, new_vs = (refs[i : i + 7] for i in range(0, 42, 7))
    factor = jnp.minimum(1.0, 0.5 * lax.rsqrt(squares_ref[:1, :1] / count + 1e-30))
    for n in range(layers):

        @pl.when(pl.program_id(0) == n)
        def _(n=n):
            for i, (which, runs) in enumerate(places):
                to = 0
                for at, size in runs:
                    here = pl.ds(to, size)
                    g = wide(grads[n][which][:, at : at + size]) * factor
                    m = 0.9 * ms[i][0, :, here] + 0.1 * g
                    v = 0.95 * vs[i][0, :, here] + 0.05 * g * g
                    w = wide(weights[i][0, :, here])
                    new_ms[i][0, :, here] = m
                    new_vs[i][0, :, here] = v
                    new_weights[i][0, :, here] = low(w - 0.02 * (m * lax.rsqrt(v + 1e-8) + 0.1 * w))
                    to += size


def update(squares, grads, weights, m, v, count, places, steps=4):
    layers = len(grads)

    def block(t):
        return pl.BlockSpec((1, t.shape[1] // steps, t.shape[2]), lambda n, i: (n, i, 0))

    def summed(t, n):
        return pl.BlockSpec((t.shape[0] // steps, t.shape[1]), lambda l, i: (jnp.where(l == n, i, jnp.where(l < n, 0, steps - 1)), 0))

    out = pl.pallas_call(
        functools.partial(update_kernel, layers=layers, count=count, places=places),
        grid=(layers, steps),
        in_specs=[pl.BlockSpec((8, 128), lambda n, i: (0, 0))]
        + [summed(t, n) for n, four in enumerate(grads) for t in four]
        + [block(t) for t in (*weights, *m, *v)],
        out_specs=[block(t) for t in (*weights, *m, *v)],
        out_shape=[jax.ShapeDtypeStruct(t.shape, t.dtype) for t in (*weights, *m, *v)],
        compiler_params=params("arbitrary", "arbitrary"),
        name="update",
    )(squares, *(t for four in grads for t in four), *weights, *m, *v)
    return tuple(out)


def solution(mesh):
    group = mesh.shape["dp"]

    def gather(w):
        return lax.all_gather(w, "dp", axis=0, tiled=True)

    def scatter(g):
        return lax.psum_scatter(g, "dp", scatter_dimension=0, tiled=True)

    def step(x, dy, *arrays):
        weights, m, v = (arrays[i : i + 7] for i in (0, 7, 14))
        wq, wk, wv, wo, wg, wu, wd = weights
        layers = wq.shape[0]
        nq, nk = wq.shape[2], wk.shape[2]
        kv, g = nk // HEAD, nq // nk
        full = []
        for n in range(layers):
            full.append((gather(stack((wq, wk, wv), wo, n)), gather(in_turns(wg, wu, n)), gather(wd[n])))
        h = x[0]
        cos, sin = tables(h.shape[0])
        kept = []
        for n in range(layers):
            stacks, wgu, wd_ = full[n]
            scale = scale_of(h)
            if n:
                scale, stacks = barrier(scale, stacks)
            wqkv, wo_ = unstack(stacks.reshape(group, -1, wo.shape[2]), wq.shape[1], nq + 2 * nk)
            full[n] = wqkv, wo_, wgu, wd_
            a = low(wide(h) * scale)
            qkv = low(dot(a, wqkv))
            o, lse = attend(qkv, cos, sin, kv, g)
            mid = h + low(dot(o, wo_))
            b = normed(mid)
            act, slope = unit(b, wgu)
            kept.append((h, a, qkv, lse, o, mid, b, act, slope))
            if n < layers - 1:
                h = mid + low(dot(act, wd_))
        by_h = dy[0]
        mine = [None] * layers
        late = []
        for n in reversed(range(layers)):
            wqkv, wo_, wgu, wd_ = full[n]
            h, a, qkv, lse, o, mid, b, act, slope = kept[n]
            by_wd = low(dot(act, by_h, 0, 0))
            by_h, by_wd = barrier(by_h, by_wd)
            got_wd = scatter(by_wd)
            by_gu, by_wgu = unit_back(by_h, wd_, slope, b)
            if late:
                by_wgu, late[0] = barrier(by_wgu, late[0])
                mine[n + 1] = tuple(late)
            got_wgu = scatter(by_wgu)
            by_b = low(dot(by_gu, wgu, 1, 1))
            by_b, got_wd = barrier(by_b, got_wd)
            by_mid = normed_back(mid, by_b, by_h)
            by_wo = low(dot(o, by_mid, 0, 0))
            by_mid, by_wo = barrier(by_mid, by_wo)
            got_wo = scatter(by_wo)
            by_o = low(dot(by_mid, wo_, 1, 1))
            by_qkv = attend_back(qkv, cos, sin, by_o, o, lse, kv, g)
            by_qkv, got_wgu = barrier(by_qkv, got_wgu)
            by_wqkv = low(dot(a, by_qkv, 0, 0))
            by_qkv, by_wqkv, got_wo = barrier(by_qkv, by_wqkv, got_wo)
            late = [scatter(by_wqkv), got_wo, got_wgu, got_wd]
            if n:
                by_a = low(dot(by_qkv, wqkv, 1, 1))
                by_h = normed_back(h, by_a, by_mid)
        mine[0] = tuple(late)
        last, *others = (t for four in mine for t in four)
        rest = sum(jnp.sum(wide(t) ** 2) for t in others)
        count = group * sum(w.size for w in weights)
        ff = wg.shape[2]
        places = ((0, ((0, nq),)), (0, ((nq, nk),)), (0, ((nq + nk, nk),)), (1, ((0, wo.shape[2]),)))
        places += tuple((2, tuple((at, TURN) for at in range(first, 2 * ff, 2 * TURN))) for first in (0, TURN))
        places += ((3, ((0, wd.shape[2]),)),)
        return update(total_of(last, rest, group), mine, weights, m, v, count, places)

    states, cut = P(("rep", "dp"), None, None), P(None, "dp", None)
    return jax.shard_map(
        step,
        mesh=mesh,
        in_specs=(states, states) + (cut,) * 21,
        out_specs=(P("rep", "dp", None),) * 21,
        check_vma=False,
    )
```

```python
import functools

import jax
import jax.numpy as jnp
from jax import lax
from jax.experimental import pallas as pl
from jax.experimental.pallas import tpu as pltpu
from jax.sharding import PartitionSpec as P

HEAD = 128
THETA = 10000
EPS = 1e-6
NEG = -1e30
HIDDEN = 2 * NEG
LOG2E = 1.4426950408889634
VMEM = 60 * 2**20


def dot(a, b, ca=1, cb=0):
    return lax.dot_general(a, b, (((ca,), (cb,)), ((), ())), preferred_element_type=jnp.float32)


def low(t):
    return t.astype(jnp.bfloat16)


def wide(t):
    return t.astype(jnp.float32)


def params(*semantics):
    return pltpu.CompilerParams(dimension_semantics=semantics, vmem_limit_bytes=VMEM)


def turn(x, cos, sin):
    return x * cos + pltpu.roll(x, HEAD // 2, 1) * sin


def gap_of(bk, cols, bq):
    return lax.rem(lax.broadcasted_iota(jnp.int32, (bk, cols), 1), bq) - lax.broadcasted_iota(jnp.int32, (bk, cols), 0)


def load_queries(q_ref, q_s, cos, sin, kv, g, part):
    for i in range(kv):
        for s in range(q_ref.shape[0] // part):
            for n in range(g):
                at, to, rows = (i * g + n) * HEAD, (s * g + n) * part, slice(s * part, (s + 1) * part)
                x = q_ref[rows, at : at + HEAD]
                q_s[i, to : to + part, :] = x if cos is None else low(turn(wide(x), cos[rows], sin[rows]))


def load_keys(k_ref, k_s, cos_ref, sin_ref, kv):
    for i in range(kv):
        k_s[i] = low(turn(wide(k_ref[:, i * HEAD : (i + 1) * HEAD]), cos_ref[...], sin_ref[...]))


def attend_kernel(q_ref, k_ref, v_ref, cos_ref, sin_ref, o_ref, lse_ref, q_s, k_s, v_s, top_s, mix_s, gap_s, *, kv, g, bq, part, strip, dstrip, scale):
    iq = pl.program_id(0)
    cols, e = g * bq, scale * LOG2E

    @pl.when(iq == 0)
    def _():
        gap_s[...] = gap_of(part, g * part, part)
        load_keys(k_ref, k_s, cos_ref, sin_ref, kv)
        for i in range(kv):
            v_s[i, :HEAD, :] = v_ref[:, i * HEAD : (i + 1) * HEAD].T
            v_s[i, HEAD:, :] = jnp.ones((8, v_s.shape[2]), v_s.dtype)

    here = pl.ds(iq * bq, bq)
    load_queries(q_ref, q_s, cos_ref[here, :], sin_ref[here, :], kv, g, part)
    top_s[...] = jnp.full(top_s.shape, NEG, jnp.float32)
    mix_s[...] = jnp.zeros(mix_s.shape, jnp.float32)

    def work(j, pieces):
        scores = []
        for i, at, size, keys, edge in pieces:
            scores.append(dot(k_s[i, pl.ds(pl.multiple_of(j * bq, bq), keys), :], q_s[i, at : at + size, :], 1, 1))
        weights, keeps = [], []
        for (i, at, size, keys, edge), s in zip(pieces, scores):
            if edge:
                col = at % (g * part)
                tail = jnp.where(gap_s[:, col : col + size] >= 0, s[keys - part :], HIDDEN)
                s = tail if keys == part else jnp.concatenate([s[: keys - part], tail], 0)
            old = top_s[i : i + 1, at : at + size]
            top = jnp.maximum(old, s.max(axis=0, keepdims=True))
            top_s[i : i + 1, at : at + size] = top
            weights.append(low(jnp.exp2((s - top) * e)))
            keeps.append(jnp.exp2((old - top) * e))
        for (i, at, size, keys, edge), p, keep in zip(pieces, weights, keeps):
            values = v_s[i, :, pl.ds(pl.multiple_of(j * bq, bq), keys)]
            mix_s[i, :, at : at + size] = mix_s[i, :, at : at + size] * keep + dot(values, p, 1, 0)

    plain = [(i, at, strip, bq, False) for i in range(kv) for at in range(0, cols, strip)]
    lax.fori_loop(0, iq, lambda j, _: work(j, plain), None)
    work(iq, [(i, at, dstrip, (at // (g * part) + 1) * part, True) for i in range(kv) for at in range(0, cols, dstrip)])
    for i in range(kv):
        total = mix_s[i, HEAD : HEAD + 1, :]
        out = mix_s[i, :HEAD, :] * (1 / total)
        lse = top_s[i : i + 1, :] * scale + jnp.log(total)
        for s in range(bq // part):
            for n in range(g):
                at, to, rows = (i * g + n) * HEAD, (s * g + n) * part, slice(s * part, (s + 1) * part)
                o_ref[rows, at : at + HEAD] = low(out[:, to : to + part].T)
                lse_ref[i, n : n + 1, rows] = lse[:, to : to + part]


def attend(qkv, cos, sin, kv, g, bq=512, part=128, strip=512, dstrip=768):
    tokens = qkv.shape[0]
    nq, nk = kv * g * HEAD, kv * HEAD
    flops = 2 * tokens * tokens * nq
    return pl.pallas_call(
        functools.partial(attend_kernel, kv=kv, g=g, bq=bq, part=part, strip=strip, dstrip=dstrip, scale=HEAD**-0.5),
        grid=(tokens // bq,),
        in_specs=[
            pl.BlockSpec((bq, nq), lambda i: (i, 0)),
            pl.BlockSpec((tokens, nk), lambda i: (0, nq // nk)),
            pl.BlockSpec((tokens, nk), lambda i: (0, nq // nk + 1)),
            pl.BlockSpec((tokens, HEAD), lambda i: (0, 0)),
            pl.BlockSpec((tokens, HEAD), lambda i: (0, 0)),
        ],
        out_specs=[pl.BlockSpec((bq, nq), lambda i: (i, 0)), pl.BlockSpec((kv, g, bq), lambda i: (0, 0, i))],
        out_shape=[jax.ShapeDtypeStruct((tokens, nq), jnp.bfloat16), jax.ShapeDtypeStruct((kv, g, tokens), jnp.float32)],
        scratch_shapes=[
            pltpu.VMEM((kv, g * bq, HEAD), jnp.bfloat16),
            pltpu.VMEM((kv, tokens, HEAD), jnp.bfloat16),
            pltpu.VMEM((kv, HEAD + 8, tokens), jnp.bfloat16),
            pltpu.VMEM((kv, g * bq), jnp.float32),
            pltpu.VMEM((kv, HEAD + 8, g * bq), jnp.float32),
            pltpu.VMEM((part, g * part), jnp.int32),
        ],
        compiler_params=params("arbitrary"),
        cost_estimate=pl.CostEstimate(flops=4 * flops, bytes_accessed=20 * 2**20, transcendentals=tokens * tokens * kv * g),
        name="attend",
    )(qkv, qkv, qkv, cos, sin)


def attend_back_kernel(q_ref, k_ref, v_ref, cos_ref, sin_ref, do_ref, o_ref, lse_ref, out_ref, q_s, do_s, k_s, kt_s, dq_s, dk_s, dv_s, gap_s, *, kv, g, bq, part, strip, dstrip, scale):
    iq = pl.program_id(0)
    cols, e = g * bq, scale * LOG2E
    nq, nk = kv * g * HEAD, kv * HEAD

    @pl.when(iq == 0)
    def _():
        gap_s[...] = gap_of(part, g * part, part)
        load_keys(k_ref, k_s, cos_ref, sin_ref, kv)
        for i in range(kv):
            kt_s[i] = k_s[i].T
        dk_s[...] = jnp.zeros_like(dk_s)
        dv_s[...] = jnp.zeros_like(dv_s)

    here = pl.ds(iq * bq, bq)
    cos, sin = cos_ref[here, :], sin_ref[here, :]
    load_queries(q_ref, q_s, cos, sin, kv, g, part)
    load_queries(do_ref, do_s, None, None, kv, g, part)
    dq_s[...] = jnp.zeros_like(dq_s)
    lses, deltas = [], []
    for i in range(kv):
        one, two = [], []
        for s in range(bq // part):
            for n in range(g):
                at, rows = (i * g + n) * HEAD, slice(s * part, (s + 1) * part)
                one.append(lse_ref[i, n : n + 1, rows])
                both = wide(do_ref[rows, at : at + HEAD]) * wide(o_ref[rows, at : at + HEAD])
                two.append(both.T.sum(axis=0, keepdims=True))
        lses.append(jnp.concatenate(one, axis=1) * LOG2E)
        deltas.append(jnp.concatenate(two, axis=1))

    def work(j, pieces):
        base = pl.multiple_of(j * bq, bq)
        qs = [q_s[i, at : at + size, :] for i, at, size, _, _ in pieces]
        dos = [do_s[i, at : at + size, :] for i, at, size, _, _ in pieces]
        scores = [dot(k_s[i, pl.ds(base, keys), :], x, 1, 1) for (i, _, _, keys, _), x in zip(pieces, qs)]
        dps = [dot(v_ref[pl.ds(base, keys), i * HEAD : (i + 1) * HEAD], x, 1, 1) for (i, _, _, keys, _), x in zip(pieces, dos)]
        for n, (i, at, size, keys, edge) in enumerate(pieces):
            here_ = pl.ds(base, keys)
            p = jnp.exp2(scores[n] * e - lses[i][:, at : at + size])
            if edge:
                col = at % (g * part)
                tail = jnp.where(gap_s[:, col : col + size] >= 0, p[keys - part :], 0.0)
                p = tail if keys == part else jnp.concatenate([p[: keys - part], tail], 0)
            ds = low(p * (dps[n] - deltas[i][:, at : at + size]))
            dv_s[i, here_, :] += dot(low(p), dos[n], 1, 0)
            dk_s[i, here_, :] += dot(ds, qs[n], 1, 0)
            dq_s[i, :, at : at + size] += dot(kt_s[i, :, here_], ds, 1, 0)

    plain = [(i, at, strip, bq, False) for i in range(kv) for at in range(0, cols, strip)]
    lax.fori_loop(0, iq, lambda j, _: work(j, plain), None)
    work(iq, [(i, at, dstrip, (at // (g * part) + 1) * part, True) for i in range(kv) for at in range(0, cols, dstrip)])
    for i in range(kv):
        for s in range(bq // part):
            for n in range(g):
                at, to = (i * g + n) * HEAD, (s * g + n) * part
                x = wide(low((dq_s[i, :, to : to + part] * scale).T))
                rows = slice(s * part, (s + 1) * part)
                out_ref[pl.ds(iq * bq + s * part, part), at : at + HEAD] = low(turn(x, cos[rows], -sin[rows]))

    @pl.when(iq == pl.num_programs(0) - 1)
    def _():
        for i in range(kv):
            at = nq + i * HEAD
            out_ref[:, at : at + HEAD] = low(turn(wide(low(dk_s[i] * scale)), cos_ref[...], -sin_ref[...]))
            out_ref[:, at + nk : at + nk + HEAD] = low(dv_s[i])


def attend_back(qkv, cos, sin, d_out, out, lse, kv, g, bq=256, part=128, strip=256, dstrip=256):
    tokens = qkv.shape[0]
    nq, nk = kv * g * HEAD, kv * HEAD
    rows = pl.BlockSpec((bq, nq), lambda i: (i, 0))
    once = pl.Buffered(1)
    table = pl.BlockSpec((tokens, HEAD), lambda i: (0, 0), pipeline_mode=once)
    return pl.pallas_call(
        functools.partial(attend_back_kernel, kv=kv, g=g, bq=bq, part=part, strip=strip, dstrip=dstrip, scale=HEAD**-0.5),
        grid=(tokens // bq,),
        in_specs=[
            rows,
            pl.BlockSpec((tokens, nk), lambda i: (0, nq // nk), pipeline_mode=once),
            pl.BlockSpec((tokens, nk), lambda i: (0, nq // nk + 1), pipeline_mode=once),
            table,
            table,
            rows,
            rows,
            pl.BlockSpec((kv, g, bq), lambda i: (0, 0, i)),
        ],
        out_specs=pl.BlockSpec(qkv.shape, lambda i: (0, 0), pipeline_mode=once),
        out_shape=jax.ShapeDtypeStruct(qkv.shape, jnp.bfloat16),
        scratch_shapes=[
            pltpu.VMEM((kv, g * bq, HEAD), jnp.bfloat16),
            pltpu.VMEM((kv, g * bq, HEAD), jnp.bfloat16),
            pltpu.VMEM((kv, tokens, HEAD), jnp.bfloat16),
            pltpu.VMEM((kv, HEAD, tokens), jnp.bfloat16),
            pltpu.VMEM((kv, HEAD, g * bq), jnp.float32),
            pltpu.VMEM((kv, tokens, HEAD), jnp.float32),
            pltpu.VMEM((kv, tokens, HEAD), jnp.float32),
            pltpu.VMEM((part, g * part), jnp.int32),
        ],
        compiler_params=params("arbitrary"),
        cost_estimate=pl.CostEstimate(flops=10 * tokens * tokens * nq, bytes_accessed=40 * 2**20, transcendentals=tokens * tokens * kv * g),
        name="attend_back",
    )(qkv, qkv, qkv, cos, sin, d_out, out, lse)


TURN = 512


def unit_kernel(b_ref, w_ref, act_ref, slope_ref, *, rows):
    for at in range(0, b_ref.shape[0], rows):
        both = dot(b_ref[at : at + rows, :], w_ref[...])
        gate, up = both[:, :TURN], both[:, TURN:]
        sig = jax.nn.sigmoid(gate)
        silu = gate * sig
        act_ref[at : at + rows, :] = low(silu * up)
        slope_ref[at : at + rows, :TURN] = up * (sig + silu * (1 - sig))
        slope_ref[at : at + rows, TURN:] = silu


def unit(b, w, bm=2048, rows=256):
    tokens, d = b.shape
    n = w.shape[1] // (2 * TURN)
    return pl.pallas_call(
        functools.partial(unit_kernel, rows=rows),
        grid=(n, tokens // bm),
        in_specs=[pl.BlockSpec((bm, d), lambda j, i: (i, 0)), pl.BlockSpec((d, 2 * TURN), lambda j, i: (0, j))],
        out_specs=[pl.BlockSpec((bm, TURN), lambda j, i: (i, j)), pl.BlockSpec((bm, 2 * TURN), lambda j, i: (i, j))],
        out_shape=[jax.ShapeDtypeStruct((tokens, n * TURN), jnp.bfloat16), jax.ShapeDtypeStruct((tokens, 2 * n * TURN), jnp.float32)],
        compiler_params=params("arbitrary", "arbitrary"),
        cost_estimate=pl.CostEstimate(flops=2 * tokens * d * w.shape[1], bytes_accessed=tokens * n * TURN * 12, transcendentals=tokens * n * TURN),
        name="unit",
    )(b, w)


def last_unit_kernel(b_ref, w_ref, dy_ref, slope_ref, by_wd_ref, act_s, turned_s, *, rows):
    unit_kernel(b_ref, w_ref, act_s, slope_ref, rows=rows)
    turned_s[...] = act_s[...].T
    for at in range(0, TURN, rows):
        by_wd_ref[at : at + rows, :] = low(dot(turned_s[at : at + rows, :], dy_ref[...]))


def last_unit(b, w, dy, rows=256):
    tokens, d = b.shape
    n = w.shape[1] // (2 * TURN)
    whole = pl.BlockSpec((tokens, d), lambda j: (0, 0))
    return pl.pallas_call(
        functools.partial(last_unit_kernel, rows=rows),
        grid=(n,),
        in_specs=[whole, pl.BlockSpec((d, 2 * TURN), lambda j: (0, j)), whole],
        out_specs=[pl.BlockSpec((tokens, 2 * TURN), lambda j: (0, j)), pl.BlockSpec((TURN, d), lambda j: (j, 0))],
        out_shape=[jax.ShapeDtypeStruct((tokens, 2 * n * TURN), jnp.float32), jax.ShapeDtypeStruct((n * TURN, d), jnp.bfloat16)],
        scratch_shapes=[pltpu.VMEM((tokens, TURN), jnp.bfloat16), pltpu.VMEM((TURN, tokens), jnp.bfloat16)],
        compiler_params=params("arbitrary"),
        cost_estimate=pl.CostEstimate(flops=3 * tokens * d * w.shape[1], bytes_accessed=tokens * n * TURN * 12, transcendentals=tokens * n * TURN),
        name="last_unit",
    )(b, w, dy)


def unit_back_kernel(dy_ref, wd_ref, slope_ref, b_ref, by_both_ref, by_w_ref, b_s, *, rows):
    @pl.when(pl.program_id(0) == 0)
    def _():
        b_s[...] = b_ref[...].T

    for at in range(0, dy_ref.shape[0], rows):
        by_act = wide(low(dot(dy_ref[at : at + rows, :], wd_ref[...], 1, 1)))
        by_both_ref[at : at + rows, :TURN] = low(by_act * slope_ref[at : at + rows, :TURN])
        by_both_ref[at : at + rows, TURN:] = low(by_act * slope_ref[at : at + rows, TURN:])
    for at in range(0, b_s.shape[0], rows):
        by_w_ref[at : at + rows, :] = low(dot(b_s[at : at + rows, :], by_both_ref[...]))


def unit_back(dy, wd, slope, b, rows=256):
    tokens, d = dy.shape
    n = wd.shape[0] // TURN
    whole = pl.BlockSpec((tokens, d), lambda j: (0, 0))
    pair = pl.BlockSpec((tokens, 2 * TURN), lambda j: (0, j))
    return pl.pallas_call(
        functools.partial(unit_back_kernel, rows=rows),
        grid=(n,),
        in_specs=[whole, pl.BlockSpec((TURN, d), lambda j: (j, 0)), pair, whole],
        out_specs=[pair, pl.BlockSpec((d, 2 * TURN), lambda j: (0, j))],
        out_shape=[jax.ShapeDtypeStruct(slope.shape, jnp.bfloat16), jax.ShapeDtypeStruct((d, slope.shape[1]), jnp.bfloat16)],
        scratch_shapes=[pltpu.VMEM((d, tokens), jnp.bfloat16)],
        compiler_params=params("arbitrary"),
        cost_estimate=pl.CostEstimate(flops=6 * tokens * d * wd.shape[0], bytes_accessed=tokens * wd.shape[0] * 14, transcendentals=0),
        name="unit_back",
    )(dy, wd, slope, b)


def norm_back_kernel(by_ref, w_ref, h_ref, by_h_ref, out_ref, sum_s, *, rows):
    k = pl.program_id(1)

    @pl.when(k == 0)
    def _():
        sum_s[...] = jnp.zeros_like(sum_s)

    for at in range(0, sum_s.shape[0], rows):
        sum_s[at : at + rows, :] += dot(by_ref[at : at + rows, :], w_ref[...], 1, 1)

    @pl.when(k == pl.num_programs(1) - 1)
    def _():
        for at in range(0, sum_s.shape[0], rows):
            here = slice(at, at + rows)
            out_ref[here, :] = normed_back(h_ref[here, :], low(sum_s[here, :]), by_h_ref[here, :])


def norm_back(by, w, h, by_h, bm=1024, bk=2048, rows=256):
    tokens, d = h.shape
    block = pl.BlockSpec((bm, d), lambda i, k: (i, 0))
    return pl.pallas_call(
        functools.partial(norm_back_kernel, rows=rows),
        grid=(tokens // bm, by.shape[1] // bk),
        in_specs=[pl.BlockSpec((bm, bk), lambda i, k: (i, k)), pl.BlockSpec((d, bk), lambda i, k: (0, k)), block, block],
        out_specs=block,
        out_shape=jax.ShapeDtypeStruct(h.shape, jnp.bfloat16),
        scratch_shapes=[pltpu.VMEM((bm, d), jnp.float32)],
        compiler_params=params("arbitrary", "arbitrary"),
        cost_estimate=pl.CostEstimate(flops=2 * by.size * d, bytes_accessed=2 * by.size + 4 * w.size + 6 * h.size, transcendentals=tokens),
        name="norm_back",
    )(by, w, h, by_h)


def barrier(*values):
    return lax.optimization_barrier(values)


def scale_of(h):
    return lax.rsqrt(jnp.mean(wide(h) ** 2, -1, keepdims=True) + EPS)


def normed(h):
    return low(wide(h) * scale_of(h))


def normed_back(h, by_out, by_h):
    x, g, scale = wide(h), wide(by_out), scale_of(h)
    through = g * scale - x * (scale**3 * jnp.mean(g * x, -1, keepdims=True))
    return low(wide(by_h) + through)


def tables(tokens):
    half = HEAD // 2
    angle = jnp.arange(tokens, dtype=jnp.float32)[:, None] * THETA ** (-jnp.arange(half, dtype=jnp.float32) / half)
    cos, sin = jnp.cos(angle), jnp.sin(angle)
    return jnp.concatenate([cos, cos], 1), jnp.concatenate([-sin, sin], 1)


def in_turns_kernel(a_ref, b_ref, out_ref):
    for at in range(0, a_ref.shape[2], TURN):
        out_ref[:, 2 * at : 2 * at + TURN] = a_ref[0, :, at : at + TURN]
        out_ref[:, 2 * at + TURN : 2 * at + 2 * TURN] = b_ref[0, :, at : at + TURN]


def in_turns(a, b, number):
    rows, columns = a.shape[1], a.shape[2]
    half = pl.BlockSpec((1, rows // 2, columns), lambda i: (number, i, 0))
    return pl.pallas_call(
        in_turns_kernel,
        grid=(2,),
        in_specs=[half, half],
        out_specs=pl.BlockSpec((rows // 2, 2 * columns), lambda i: (i, 0)),
        out_shape=jax.ShapeDtypeStruct((rows, 2 * columns), a.dtype),
        compiler_params=params("arbitrary"),
        name="in_turns",
    )(a, b)


def stack_kernel(*refs):
    *parts, below_ref, out_ref = refs
    rows, width = parts[0].shape[1], out_ref.shape[1]
    to = 0
    for part in parts:
        for at in range(0, part.shape[2], HEAD):
            piece, column = divmod(to, width)
            out_ref[piece * rows : (piece + 1) * rows, column : column + HEAD] = part[0, :, at : at + HEAD]
            to += HEAD
    out_ref[to // width * rows :, :] = below_ref[0]


def stack(parts, below, number):
    rows, width = parts[0].shape[1], below.shape[2]
    height = rows * sum(t.shape[2] for t in parts) // width + below.shape[1]
    return pl.pallas_call(
        stack_kernel,
        grid=(1,),
        in_specs=[pl.BlockSpec((1, *t.shape[1:]), lambda i: (number, 0, 0)) for t in (*parts, below)],
        out_specs=pl.BlockSpec((height, width), lambda i: (0, 0)),
        out_shape=jax.ShapeDtypeStruct((height, width), below.dtype),
        compiler_params=params("arbitrary"),
        name="stack",
    )(*parts, below)


def unstack(t, rows, columns):
    group, _, width = t.shape
    pieces = [t[:, at : at + rows].reshape(group * rows, width) for at in range(0, rows * columns // width, rows)]
    return jnp.concatenate(pieces, 1), t[:, rows * columns // width :].reshape(-1, width)


def total_kernel(last_ref, rest_ref, out_ref, mine_s, all_s, send_sem, recv_sem, *, n):
    me = lax.axis_index("dp")
    last = wide(last_ref[...])
    mine_s[...] = rest_ref[...] + jnp.sum(last * last, keepdims=True)
    entry = pltpu.get_barrier_semaphore()
    for k in range(1, n):
        pl.semaphore_signal(entry, inc=1, device_id={"dp": lax.rem(me + k, n)}, device_id_type=pl.DeviceIdType.MESH)
    pl.semaphore_wait(entry, n - 1)
    copies = []
    for k in range(1, n):
        copies.append(
            pltpu.make_async_remote_copy(
                src_ref=mine_s,
                dst_ref=all_s.at[k],
                send_sem=send_sem.at[k],
                recv_sem=recv_sem.at[k],
                device_id={"dp": lax.rem(me + k, n)},
                device_id_type=pl.DeviceIdType.MESH,
            )
        )
    for copy in copies:
        copy.start()
    for copy in copies:
        copy.wait()
    total = mine_s[...]
    for k in range(1, n):
        total = total + all_s[k]
    out_ref[...] = total


def total_of(last, rest, n):
    return pl.pallas_call(
        functools.partial(total_kernel, n=n),
        in_specs=[pl.BlockSpec(memory_space=pltpu.VMEM)] * 2,
        out_specs=pl.BlockSpec(memory_space=pltpu.VMEM),
        out_shape=jax.ShapeDtypeStruct((8, 128), jnp.float32),
        scratch_shapes=[
            pltpu.VMEM((8, 128), jnp.float32),
            pltpu.VMEM((n, 8, 128), jnp.float32),
            pltpu.SemaphoreType.DMA((n,)),
            pltpu.SemaphoreType.DMA((n,)),
        ],
        compiler_params=pltpu.CompilerParams(collective_id=0, has_side_effects=True),
        name="total",
    )(last, jnp.broadcast_to(rest, (8, 128)))


def update_kernel(squares_ref, *refs, layers, count, places):
    grads, refs = [refs[4 * n : 4 * n + 4] for n in range(layers)], refs[4 * layers :]
    weights, ms, vs, new_weights, new_ms, new_vs = (refs[i : i + 7] for i in range(0, 42, 7))
    factor = jnp.minimum(1.0, 0.5 * lax.rsqrt(squares_ref[:1, :1] / count + 1e-30))
    for n in range(layers):

        @pl.when(pl.program_id(0) == n)
        def _(n=n):
            for i, (which, runs) in enumerate(places):
                to = 0
                for at, size in runs:
                    here = pl.ds(to, size)
                    g = wide(grads[n][which][:, at : at + size]) * factor
                    m = 0.9 * ms[i][0, :, here] + 0.1 * g
                    v = 0.95 * vs[i][0, :, here] + 0.05 * g * g
                    w = wide(weights[i][0, :, here])
                    new_ms[i][0, :, here] = m
                    new_vs[i][0, :, here] = v
                    new_weights[i][0, :, here] = low(w - 0.02 * (m * lax.rsqrt(v + 1e-8) + 0.1 * w))
                    to += size


def update(squares, grads, weights, m, v, count, places, steps=4):
    layers = len(grads)

    def block(t):
        return pl.BlockSpec((1, t.shape[1] // steps, t.shape[2]), lambda n, i: (n, i, 0))

    def summed(t, n):
        return pl.BlockSpec((t.shape[0] // steps, t.shape[1]), lambda l, i: (jnp.where(l == n, i, jnp.where(l < n, 0, steps - 1)), 0))

    out = pl.pallas_call(
        functools.partial(update_kernel, layers=layers, count=count, places=places),
        grid=(layers, steps),
        in_specs=[pl.BlockSpec((8, 128), lambda n, i: (0, 0))]
        + [summed(t, n) for n, four in enumerate(grads) for t in four]
        + [block(t) for t in (*weights, *m, *v)],
        out_specs=[block(t) for t in (*weights, *m, *v)],
        out_shape=[jax.ShapeDtypeStruct(t.shape, t.dtype) for t in (*weights, *m, *v)],
        compiler_params=params("arbitrary", "arbitrary"),
        name="update",
    )(squares, *(t for four in grads for t in four), *weights, *m, *v)
    return tuple(out)


def solution(mesh):
    group = mesh.shape["dp"]

    def gather(w):
        return lax.all_gather(w, "dp", axis=0, tiled=True)

    def scatter(g):
        return lax.psum_scatter(g, "dp", scatter_dimension=0, tiled=True)

    def step(x, dy, *arrays):
        weights, m, v = (arrays[i : i + 7] for i in (0, 7, 14))
        wq, wk, wv, wo, wg, wu, wd = weights
        layers = wq.shape[0]
        nq, nk = wq.shape[2], wk.shape[2]
        kv, g = nk // HEAD, nq // nk
        full = []
        for n in range(layers):
            full.append((gather(stack((wq, wk, wv), wo, n)), gather(in_turns(wg, wu, n)), gather(wd[n])))
        h = x[0]
        cos, sin = tables(h.shape[0])
        kept = []
        for n in range(layers):
            stacks, wgu, wd_ = full[n]
            scale = scale_of(h)
            if n:
                scale, stacks = barrier(scale, stacks)
            wqkv, wo_ = unstack(stacks.reshape(group, -1, wo.shape[2]), wq.shape[1], nq + 2 * nk)
            full[n] = wqkv, wo_, wgu, wd_
            a = low(wide(h) * scale)
            qkv = low(dot(a, wqkv))
            o, lse = attend(qkv, cos, sin, kv, g)
            mid = h + low(dot(o, wo_))
            b = normed(mid)
            if n < layers - 1:
                act, slope = unit(b, wgu)
                kept.append((h, a, qkv, lse, o, mid, b, act, slope))
                h = mid + low(dot(act, wd_))
            else:
                slope, by_wd = last_unit(b, wgu, dy[0])
                kept.append((h, a, qkv, lse, o, mid, b, None, slope))
        by_h = dy[0]
        mine = [None] * layers
        late = []
        for n in reversed(range(layers)):
            wqkv, wo_, wgu, wd_ = full[n]
            h, a, qkv, lse, o, mid, b, act, slope = kept[n]
            if n < layers - 1:
                by_wd = low(dot(act, by_h, 0, 0))
            by_h, by_wd = barrier(by_h, by_wd)
            got_wd = scatter(by_wd)
            by_gu, by_wgu = unit_back(by_h, wd_, slope, b)
            if late:
                by_wgu, late[0] = barrier(by_wgu, late[0])
                mine[n + 1] = tuple(late)
            got_wgu = scatter(by_wgu)
            by_mid = norm_back(by_gu, wgu, mid, by_h)
            by_mid, got_wd = barrier(by_mid, got_wd)
            by_wo = low(dot(o, by_mid, 0, 0))
            by_mid, by_wo = barrier(by_mid, by_wo)
            got_wo = scatter(by_wo)
            by_o = low(dot(by_mid, wo_, 1, 1))
            by_qkv = attend_back(qkv, cos, sin, by_o, o, lse, kv, g)
            by_qkv, got_wgu = barrier(by_qkv, got_wgu)
            by_wqkv = low(dot(a, by_qkv, 0, 0))
            by_qkv, by_wqkv, got_wo = barrier(by_qkv, by_wqkv, got_wo)
            late = [scatter(by_wqkv), got_wo, got_wgu, got_wd]
            if n:
                by_a = low(dot(by_qkv, wqkv, 1, 1))
                by_h = normed_back(h, by_a, by_mid)
        mine[0] = tuple(late)
        last, *others = (t for four in mine for t in four)
        rest = sum(jnp.sum(wide(t) ** 2) for t in others)
        count = group * sum(w.size for w in weights)
        ff = wg.shape[2]
        places = ((0, ((0, nq),)), (0, ((nq, nk),)), (0, ((nq + nk, nk),)), (1, ((0, wo.shape[2]),)))
        places += tuple((2, tuple((at, TURN) for at in range(first, 2 * ff, 2 * TURN))) for first in (0, TURN))
        places += ((3, ((0, wd.shape[2]),)),)
        return update(total_of(last, rest, group), mine, weights, m, v, count, places)

    states, cut = P(("rep", "dp"), None, None), P(None, "dp", None)
    return jax.shard_map(
        step,
        mesh=mesh,
        in_specs=(states, states) + (cut,) * 21,
        out_specs=(P("rep", "dp", None),) * 21,
        check_vma=False,
    )
```
